32 devices in a mesh: batch: 2 (over y), space: 8 (over z, x), hidden: 2 (over core).
Axes of the slice: x: 2, y: 2, z: 4, core: 2. Of those that a mesh axis runs over, the one named last changes fastest.
Arguments:
- nodes: bfloat16 [2, 1024, 512], P('batch', 'space'), may hold values from -6 to 6
- edges: bfloat16 [2, 8192, 512], P('batch', 'space'), may hold values from -6 to 6
- node_cotangent: bfloat16 [2, 1024, 512], P('batch', 'space'), may hold values from -18 to 18
- edge_cotangent: bfloat16 [2, 8192, 512], P('batch', 'space'), may hold values from -18 to 18
- senders: int32 [8192], P('space'), may hold values from 0 to 255
- receivers: int32 [8192], P('space'), may hold values from 0 to 127
- send_lists: int32 [8, 2, 64], P('space'), may hold values from 0 to 127
- edge_first: bfloat16 [1536, 512], P(None, 'hidden'), may hold values from -0.15625 to 0.15625
- edge_bias: float32 [512], P('hidden'), may hold values from -3 to 3
- edge_second: bfloat16 [512, 512], P('hidden'), may hold values from -0.25 to 0.25
- edge_gain: float32 [512], replicated, may hold values from 0.1 to 1.9
- node_first: bfloat16 [1024, 512], replicated, may hold values from -0.1875 to 0.1875
- node_bias: float32 [512], replicated, may hold values from -3 to 3
- node_second: bfloat16 [512, 512], replicated, may hold values from -0.25 to 0.25
- node_gain: float32 [512], replicated, may hold values from 0.1 to 1.9
Outputs:
- grad_nodes: bfloat16 [2, 1024, 512], P('batch', 'space', 'hidden')
- grad_edges: bfloat16 [2, 8192, 512], P('batch', 'space', 'hidden')
- grad_edge_first: float32 [1536, 512], P(None, 'hidden')
- grad_edge_bias: float32 [512], P('hidden')
- grad_edge_second: float32 [512, 512], P('hidden')
- grad_edge_gain: float32 [512], replicated
- grad_node_first: float32 [1024, 512], replicated
- grad_node_bias: float32 [512], replicated
- grad_node_second: float32 [512, 512], replicated
- grad_node_gain: float32 [512], replicated
The draws below stay inside these ranges and needn't reach their ends.
Inputs may be any that keep to these rules, and one draw needn't show every extreme that they name: `senders`: an entry below 128 is a local node of the edge's patch; 128 + k is row k of the previous patch's list 1, 192 + k row k of the next patch's list 0. `receivers`: local nodes of the edge's patch. `send_lists`: local nodes of the patch; entries may repeat.
All inputs are finite; a program needn't handle non-finite values.
Results may differ from the reference program's by a relative error of at most 0.015.
Values may be sent and summed in bfloat16 or wider, within the bound.
A program may use at most 128 MiB of HBM per device.

```python
import jax
import jax.numpy as jnp
from jax import lax

D = 512
FF = 512
NODE_DEV = 128
HALO = 64
EDGE_DEV = 1024
TAB = 256
PATCHES = 8
NODES = 1024
EDGES = 8192
SAMPLES = 2


def rising_rows(key, row_count, width):
    first_key = jax.random.fold_in(key, 0)
    ramp = 1.0 + 2.0 * jnp.arange(row_count, dtype=jnp.float32) / row_count
    base = jnp.clip(jax.random.normal(first_key, (SAMPLES, row_count, width), jnp.float32), -6.0, 6.0)
    return base * ramp[None, :, None]


def draw_node_cotangent(key, part):
    return rising_rows(jax.random.fold_in(key, 7), NODES, D).astype(jnp.bfloat16)


def draw_edge_cotangent(key, part):
    return rising_rows(jax.random.fold_in(key, 11), EDGES, D).astype(jnp.bfloat16)


def plant(values, own_key, least, largest):
    spot = [jax.random.randint(jax.random.fold_in(own_key, axis), (), 0, length) for axis, length in enumerate(values.shape)]
    widest = values.shape.index(max(values.shape))
    neighbour = spot[:widest] + [(spot[widest] + 1) % values.shape[widest]] + spot[widest + 1:]
    return values.at[tuple(spot)].set(least).at[tuple(neighbour)].set(largest)


def levels(own_key, dims, cuts, low, top_value):
    level, own = 1.0, jax.random.fold_in(own_key, 6)
    for position, shards_of in cuts:
        steps = jnp.exp(jax.random.uniform(jax.random.fold_in(own, position), (shards_of,), jnp.float32, low / len(cuts), top_value / len(cuts)))
        level = level * jnp.repeat(steps, dims[position] // shards_of).reshape([-1 if axis == position else 1 for axis in range(len(dims))])
    return level


def normal_values(rng, dims, spread, most, pieces=(), held_as=jnp.bfloat16):
    drawn = spread * jax.random.normal(rng, dims, jnp.float32)
    if pieces:
        drawn = drawn * levels(rng, dims, pieces, -0.22, 0.18)
    return jnp.clip(drawn, -most, most).astype(held_as)


def setup_inputs(seed: int = 0) -> dict:
    seeds = jax.random.split(jax.random.key(seed), 16)
    nodes = normal_values(seeds[0], (SAMPLES, NODES, D), 1.0, 6.0, ((0, 2), (1, 8)))
    edges = normal_values(seeds[1], (SAMPLES, EDGES, D), 1.0, 6.0, ((0, 2), (1, 8)))
    node_cotangent = draw_node_cotangent(jax.random.fold_in(seeds[15], 71), 0)
    edge_cotangent = draw_edge_cotangent(jax.random.fold_in(seeds[15], 71), 0)
    senders = plant(jax.random.randint(seeds[4], (EDGES,), 0, TAB), jax.random.fold_in(seeds[4], 1), 0, TAB - 1).astype(jnp.int32)
    receivers = plant(jax.random.randint(seeds[5], (EDGES,), 0, NODE_DEV), jax.random.fold_in(seeds[5], 1), 0, NODE_DEV - 1).astype(jnp.int32)
    send_lists = plant(jax.random.randint(seeds[6], (PATCHES, 2, HALO), 0, NODE_DEV), jax.random.fold_in(seeds[6], 1), 0, NODE_DEV - 1).astype(jnp.int32)
    edge_first = normal_values(seeds[7], (3 * D, FF), (3 * D) ** -0.5, 0.15625, ((1, 2),))
    edge_bias = normal_values(seeds[8], (FF,), 0.5, 3.0, ((0, 2),), jnp.float32)
    edge_second = normal_values(seeds[9], (FF, D), FF ** -0.5, 0.25, ((0, 2),))
    edge_gain = jnp.clip(1.0 + 0.18 * jax.random.normal(seeds[10], (D,), jnp.float32), 0.1, 1.9)
    node_first = normal_values(seeds[11], (2 * D, FF), (2 * D) ** -0.5, 0.1875)
    node_bias = normal_values(seeds[12], (FF,), 0.5, 3.0, (), jnp.float32)
    node_second = normal_values(seeds[13], (FF, D), FF ** -0.5, 0.25)
    node_gain = jnp.clip(1.0 + 0.18 * jax.random.normal(seeds[14], (D,), jnp.float32), 0.1, 1.9)
    return {"nodes": nodes, "edges": edges, "node_cotangent": node_cotangent, "edge_cotangent": edge_cotangent, "senders": senders, "receivers": receivers, "send_lists": send_lists, "edge_first": edge_first, "edge_bias": edge_bias, "edge_second": edge_second, "edge_gain": edge_gain, "node_first": node_first, "node_bias": node_bias, "node_second": node_second, "node_gain": node_gain}


EPS = 1e-05

def matmul(lefthand, righthand):
    return jnp.dot(lefthand, righthand, preferred_element_type=jnp.float32)

def matmul_tn(lefthand, righthand):
    return lax.dot_general(lefthand, righthand, (((0,), (0,)), ((), ())), preferred_element_type=jnp.float32)

def matmul_nt(lefthand, righthand):
    return lax.dot_general(lefthand, righthand, (((1,), (1,)), ((), ())), preferred_element_type=jnp.float32)

def normalize(values):
    centre = values - lax.optimization_barrier(jnp.mean(values, axis=-1, keepdims=True))
    scaled = lax.rsqrt(lax.optimization_barrier(jnp.mean(centre * centre, axis=-1, keepdims=True)) + EPS)
    return (centre * scaled, scaled)

def norm_back(upstream, gain_vec, normed, scaled):
    pulled = upstream * gain_vec
    return scaled * (pulled - lax.optimization_barrier(jnp.mean(pulled, axis=-1, keepdims=True)) - normed * lax.optimization_barrier(jnp.mean(pulled * normed, axis=-1, keepdims=True)))

def silu_slope(values):
    logistic = jax.nn.sigmoid(values)
    return logistic * (1.0 + values * (1.0 - logistic))

def reference(nodes, edges, node_cotangent, edge_cotangent, senders, receivers, send_lists, edge_first, edge_bias, edge_second, edge_gain, node_first, node_bias, node_second, node_gain):
    samples = nodes.shape[0]
    patch_ids = jnp.arange(PATCHES, dtype=jnp.int32)[:, None]
    sample_ids = jnp.arange(samples, dtype=jnp.int32)[:, None]
    node_blocks = nodes.reshape(samples, PATCHES, NODE_DEV, D)
    send_ids = senders.reshape(PATCHES, EDGE_DEV)
    recv_ids = receivers.reshape(PATCHES, EDGE_DEV)
    to_prev = node_blocks[:, patch_ids, send_lists[:, 0, :]]
    to_next = node_blocks[:, patch_ids, send_lists[:, 1, :]]
    table = jnp.concatenate([node_blocks, jnp.roll(to_next, 1, axis=1), jnp.roll(to_prev, -1, axis=1)], axis=2)
    from_sender = table[:, patch_ids, send_ids]
    from_receiver = node_blocks[:, patch_ids, recv_ids]
    edge_blocks = edges.reshape(samples, PATCHES, EDGE_DEV, D)
    edge_input = jnp.concatenate([edge_blocks, from_sender, from_receiver], axis=3).reshape(-1, 3 * D)
    edge_pre = matmul(edge_input, edge_first) + edge_bias
    edge_act = jax.nn.silu(edge_pre).astype(jnp.bfloat16)
    edge_normed, edge_scale = normalize(matmul(edge_act, edge_second))
    message = (edge_gain * edge_normed).astype(jnp.bfloat16)
    flat_recv = (patch_ids * NODE_DEV + recv_ids).reshape(-1)
    segment_ids = (sample_ids * NODES + flat_recv[None, :]).reshape(-1)
    gathered = jax.ops.segment_sum(message.astype(jnp.float32), segment_ids, num_segments=samples * NODES).astype(jnp.bfloat16)
    node_input = jnp.concatenate([nodes.reshape(-1, D), gathered], axis=1)
    node_pre = matmul(node_input, node_first) + node_bias
    node_act = jax.nn.silu(node_pre).astype(jnp.bfloat16)
    node_normed, node_scale = normalize(matmul(node_act, node_second))
    node_upstream = node_cotangent.reshape(-1, D).astype(jnp.float32)
    grad_node_gain = lax.optimization_barrier(jnp.sum(node_upstream * node_normed, axis=0))
    node_dz = norm_back(node_upstream, node_gain, node_normed, node_scale).astype(jnp.bfloat16)
    grad_node_second = matmul_tn(node_act, node_dz)
    node_dh = (matmul_nt(node_dz, node_second) * silu_slope(node_pre)).astype(jnp.bfloat16)
    grad_node_first = matmul_tn(node_input, node_dh)
    grad_node_bias = lax.optimization_barrier(jnp.sum(node_dh.astype(jnp.float32), axis=0))
    node_dx = matmul_nt(node_dh, node_first)
    agg_grad = node_dx[:, D:].astype(jnp.bfloat16)
    edge_upstream = edge_cotangent.reshape(-1, D).astype(jnp.float32)
    message_grad = edge_upstream + agg_grad[segment_ids].astype(jnp.float32)
    grad_edge_gain = lax.optimization_barrier(jnp.sum(message_grad * edge_normed, axis=0))
    edge_dz = norm_back(message_grad, edge_gain, edge_normed, edge_scale).astype(jnp.bfloat16)
    grad_edge_second = matmul_tn(edge_act, edge_dz)
    edge_dh = (matmul_nt(edge_dz, edge_second) * silu_slope(edge_pre)).astype(jnp.bfloat16)
    grad_edge_first = matmul_tn(edge_input, edge_dh)
    grad_edge_bias = lax.optimization_barrier(jnp.sum(edge_dh.astype(jnp.float32), axis=0))
    edge_part = matmul_nt(edge_dh, edge_first[:D])
    grad_edges = (edge_upstream + edge_part).astype(jnp.bfloat16).reshape(samples, EDGES, D)
    send_part = matmul_nt(edge_dh, edge_first[D:2 * D])
    table_ids = (sample_ids * (PATCHES * TAB) + (patch_ids * TAB + send_ids).reshape(-1)[None, :]).reshape(-1)
    table_grad = jax.ops.segment_sum(send_part, table_ids, num_segments=samples * PATCHES * TAB).reshape(samples, PATCHES, TAB, D)
    recv_part = matmul_nt(edge_dh, edge_first[2 * D:])
    recv_grad = jax.ops.segment_sum(recv_part, segment_ids, num_segments=samples * NODES).reshape(samples, PATCHES, NODE_DEV, D)
    own_grad = table_grad[:, :, :NODE_DEV] + recv_grad
    back_prev = jnp.roll(table_grad[:, :, NODE_DEV + HALO:], 1, axis=1)
    back_next = jnp.roll(table_grad[:, :, NODE_DEV:NODE_DEV + HALO], -1, axis=1)
    own_grad = own_grad.at[:, patch_ids, send_lists[:, 0, :]].add(back_prev)
    own_grad = own_grad.at[:, patch_ids, send_lists[:, 1, :]].add(back_next)
    grad_nodes = (node_upstream + node_dx[:, :D] + own_grad.reshape(-1, D)).astype(jnp.bfloat16).reshape(samples, NODES, D)
    return (grad_nodes, grad_edges, grad_edge_first, grad_edge_bias, grad_edge_second, grad_edge_gain, grad_node_first, grad_node_bias, grad_node_second, grad_node_gain)
```

```python
import functools

import jax
import jax.numpy as jnp
from jax import lax
from jax.experimental import pallas as pl
from jax.experimental.pallas import tpu as pltpu
from jax.sharding import PartitionSpec as P

EPS = 1e-05
CHUNK = 128
F32, BF16 = jnp.float32, jnp.bfloat16
MESH = pl.DeviceIdType.MESH


def mm(lefthand, righthand):
    return jnp.dot(lefthand, righthand, preferred_element_type=F32)


def mm_tn(lefthand, righthand):
    return lax.dot_general(
        lefthand, righthand, (((0,), (0,)), ((), ())), preferred_element_type=F32
    )


def mm_nt(lefthand, righthand):
    return lax.dot_general(
        lefthand, righthand, (((1,), (1,)), ((), ())), preferred_element_type=F32
    )


def normalize(values):
    centre = values - jnp.mean(values, axis=-1, keepdims=True)
    scaled = lax.rsqrt(jnp.mean(centre * centre, axis=-1, keepdims=True) + EPS)
    return centre * scaled, scaled


def norm_back(upstream, gain, normed, scaled):
    pulled = upstream * gain
    return scaled * (
        pulled
        - jnp.mean(pulled, axis=-1, keepdims=True)
        - normed * jnp.mean(pulled * normed, axis=-1, keepdims=True)
    )


def sigmoid(values):
    return 1.0 / (1.0 + jnp.exp(-values))


class Copies:
    def __init__(self, local_sems, send_sems, recv_sems):
        self.local_sems, self.send_sems, self.recv_sems = local_sems, send_sems, recv_sems
        self.locals, self.remotes = 0, 0

    def local(self, src, dst):
        copy = pltpu.make_async_copy(src, dst, self.local_sems.at[self.locals])
        self.locals += 1
        copy.start()
        return copy

    def remote(self, src, dst, device):
        copy = pltpu.make_async_remote_copy(
            src_ref=src,
            dst_ref=dst,
            send_sem=self.send_sems.at[self.remotes],
            recv_sem=self.recv_sems.at[self.remotes],
            device_id=device,
            device_id_type=MESH,
        )
        self.remotes += 1
        copy.start()
        return copy


class Reduction:
    def __init__(self, copies, buf, landing, result, rows, steps):
        self.copies, self.buf, self.landing, self.result = copies, buf, landing, result
        self.steps = steps
        self.size = rows
        self.offset = 0
        self.land = 0
        self.trail = []
        self.flight = None

    def _rows(self, start, size):
        return pl.ds(pl.multiple_of(start, 16), size)

    def send_half(self, index):
        device, bit = self.steps[index]
        half = self.size // 2
        theirs = self.offset + (1 - bit) * half
        self.flight = self.copies.remote(
            self.buf.at[self._rows(theirs, half)],
            self.landing.at[pl.ds(self.land, half)],
            device,
        )

    def take_half(self, index):
        device, bit = self.steps[index]
        half = self.size // 2
        self.flight.wait()
        mine = self.offset + bit * half
        block = 64
        while half % block:
            block //= 2
        land = self.land
        target = self.result if index + 1 == len(self.steps) else self.buf

        def add(i, carry):
            here = pl.ds(pl.multiple_of(mine + i * block, 16), block)
            there = pl.ds(pl.multiple_of(land + i * block, 16), block)
            target[here, :] = (
                self.buf[here, :].astype(F32) + self.landing[there, :].astype(F32)
            ).astype(BF16)
            return carry

        lax.fori_loop(0, half // block, add, 0)
        self.trail.append((self.offset, self.size))
        self.offset, self.size, self.land = mine, half, land + half

    def send_own(self, index):
        device, _ = self.steps[index]
        rows = self._rows(self.offset, self.size)
        self.flight = self.copies.remote(self.result.at[rows], self.result.at[rows], device)

    def take_own(self):
        self.flight.wait()
        self.offset, self.size = self.trail.pop()


def kernel(
    sizes,
    nodes_h, edges_h, ncot_h, ecot_h, senders_v, receivers_v, lists_v,
    first_h, ebias_v, second_h, egain_v, nfirst_h, nbias_v, nsecond_h, ngain_v,
    gn_out, ge_out, ng_out, eg_out, vec_out,
    nodes, edges, ncot, ecot, w1, w2, n1, n2,
    table, outgoing, oht, oh, pre, act, normed, scales, msg, agg, nin, nact, dz, dh,
    gfirst, gfirst_send, gsecond, gsecond_send, first_in, second_in,
    spart, s_send, s_in, ge_half, ge_full, back, arriving, gnode,
    ng, n_work, n_land, eg, e_work, e_land, vec, vec_in,
    local_sems, send_sems, recv_sems,
):
    batches, patches, node_rows_padded, edge_rows_padded = sizes
    b, p, h = lax.axis_index("batch"), lax.axis_index("space"), lax.axis_index("hidden")
    other = 1 - h
    partner = (b, p, other)
    prev = (b, lax.rem(p + patches - 1, patches), h)
    after = (b, lax.rem(p + 1, patches), h)
    n_count, width = nodes.shape
    e_count = edges.shape[0]
    half = width // 2
    halo = lists_v.shape[1] // 2
    t_rows = table.shape[0]
    hid = w2.shape[0]
    hhalf = hid // 2

    def flip_space(bit_index):
        stride = 1 << bit_index
        bit = lax.rem(p // stride, 2)
        return (b, p + stride * (1 - 2 * bit), h), bit

    def flip_batch():
        return (1 - b, p, h), b

    bits = patches.bit_length() - 1
    rest = [flip_space(i) for i in range(1, bits)]
    near, far = flip_space(0), flip_batch()
    pn = p + (1 - 2 * lax.rem(p, 2))
    one = ((b * (1 - h) + (1 - b) * h, pn * (1 - h) + p * h, h), near[1] * (1 - h) + far[1] * h)
    two = (((1 - b) * (1 - h) + b * h, p * (1 - h) + pn * h, h), far[1] * (1 - h) + near[1] * h)
    steps = [one, two] + rest

    copies = Copies(local_sems, send_sems, recv_sems)
    my_rows = pl.ds(pl.multiple_of(h * e_count, 128), e_count)
    my_hidden = pl.ds(pl.multiple_of(h * hhalf, 128), hhalf)
    c_nodes = copies.local(nodes_h, nodes)
    c_w1 = copies.local(first_h, w1.at[:, my_hidden])
    c_edges = copies.local(edges_h.at[my_rows], edges)
    c_w2 = copies.local(second_h, w2.at[my_hidden])
    c_n1 = copies.local(nfirst_h, n1)
    c_n2 = copies.local(nsecond_h, n2)
    c_ncot = copies.local(ncot_h, ncot)
    c_ecot = copies.local(ecot_h.at[my_rows], ecot)

    barrier = pltpu.get_barrier_semaphore()
    friends = [partner, prev, after] + [device for device, _ in steps]
    for device in friends:
        pl.semaphore_signal(barrier, inc=1, device_id=device, device_id_type=MESH)
    c_nodes.wait()
    pick_t = (
        lax.broadcasted_iota(jnp.int32, (n_count, 2 * halo), 0) == lists_v[...]
    ).astype(BF16)
    outgoing[...] = mm_tn(pick_t, nodes[...]).astype(BF16)
    pl.semaphore_wait(barrier, len(friends))
    r_w1 = copies.remote(first_h, w1.at[:, my_hidden], partner)
    r_w2 = copies.remote(second_h, w2.at[my_hidden], partner)
    r_prev = copies.remote(
        outgoing.at[pl.ds(0, halo)], table.at[pl.ds(n_count + halo, halo)], prev
    )
    r_next = copies.remote(outgoing.at[pl.ds(halo, halo)], table.at[pl.ds(n_count, halo)], after)
    table[pl.ds(0, n_count), :] = nodes[...]
    oht[pl.ds(0, t_rows), :] = (
        lax.broadcasted_iota(jnp.int32, (t_rows, e_count), 0) == senders_v[...]
    ).astype(BF16)
    oht[pl.ds(t_rows, n_count), :] = (
        lax.broadcasted_iota(jnp.int32, (n_count, e_count), 0) == receivers_v[...]
    ).astype(BF16)
    oh[...] = oht[...].astype(F32).T.astype(BF16)

    c_w1.wait()
    c_w2.wait()
    r_w1.wait()
    p_recv = mm(nodes[...], w1[2 * width :, :]).astype(BF16)
    c_edges.wait()
    for i in range(0, e_count, CHUNK):
        rows = pl.ds(i, CHUNK)
        pre[rows, :] = (
            mm(edges[rows, :], w1[:width, :]) + mm(oh[rows, t_rows:], p_recv) + ebias_v[...]
        )
    r_prev.wait()
    r_next.wait()
    r_w2.wait()
    p_send = mm(table[...], w1[width : 2 * width, :]).astype(BF16)
    for i in range(0, e_count, CHUNK):
        rows = pl.ds(i, CHUNK)
        value = pre[rows, :] + mm(oh[rows, :t_rows], p_send)
        pre[rows, :] = value
        active = (value * sigmoid(value)).astype(BF16)
        act[rows, :] = active
        norm, scale = normalize(mm(active, w2[...]))
        normed[rows, :] = norm
        scales[rows, :] = jnp.broadcast_to(scale, (CHUNK, 128))
        msg[rows, :] = (egain_v[...] * norm).astype(BF16)
    agg[0] = mm(oht[t_rows:, :], msg[...])
    r_agg = copies.remote(agg.at[0], agg.at[1], partner)
    c_n1.wait()
    c_n2.wait()
    c_ncot.wait()
    node_half = mm(nodes[...], n1[:width, :]) + nbias_v[...]
    nin[0] = nodes[...]
    r_agg.wait()
    gathered = (agg[0] + agg[1]).astype(BF16)
    nin[1] = gathered

    n_pre = node_half + mm(gathered, n1[width:, :])
    n_sig = sigmoid(n_pre)
    n_active = (n_pre * n_sig).astype(BF16)
    nact[...] = n_active
    n_norm, n_scale = normalize(mm(n_active, n2[...]))
    n_up = ncot[...].astype(F32)
    first_core = (1 - h).astype(F32)
    vec[...] = jnp.zeros_like(vec)
    vec[3:4, :] = jnp.sum(n_up * n_norm, axis=0, keepdims=True) * first_core
    n_dz = norm_back(n_up, ngain_v[...], n_norm, n_scale).astype(BF16)
    n_slope = n_sig * (1.0 + n_pre * (1.0 - n_sig))
    n_dh = (mm_nt(n_dz, n2[...]) * n_slope).astype(BF16)
    vec[2:3, :] = jnp.sum(n_dh.astype(F32), axis=0, keepdims=True) * first_core
    agg_grad = mm_nt(n_dh, n1[width:, :]).astype(BF16)
    my_feat = pl.ds(pl.multiple_of(h * half, 128), half)
    gnode[...] = ncot[:, my_feat].astype(F32) + mm_nt(n_dh, n1[my_feat, :])
    ngh = n_work
    grad = mm_tn(nin[h], n_dh).astype(BF16)
    for j in range(2):
        ngh[pl.ds(j * width, width), :] = grad[:, j * half : (j + 1) * half]
    grad = mm_tn(nact[:, my_hidden], n_dz).astype(BF16)
    for j in range(2):
        ngh[pl.ds(2 * width + j * hhalf, hhalf), :] = grad[:, j * half : (j + 1) * half]
    filled = 2 * width + 2 * hhalf
    if node_rows_padded > filled:
        ngh[pl.ds(filled, node_rows_padded - filled), :] = jnp.zeros(
            (node_rows_padded - filled, half), BF16
        )
    node_red = Reduction(copies, n_work, n_land, ng.at[h], node_rows_padded, steps)
    node_red.send_half(0)

    c_ecot.wait()
    gain_sum = jnp.zeros((1, width), F32)
    bias_sum = jnp.zeros((1, hid), F32)
    for i in range(0, e_count, CHUNK):
        rows = pl.ds(i, CHUNK)
        upstream = ecot[rows, :].astype(F32)
        norm = normed[rows, :]
        grad = upstream + mm(oh[rows, t_rows:], agg_grad)
        gain_sum = gain_sum + jnp.sum(grad * norm, axis=0, keepdims=True)
        d_z = norm_back(grad, egain_v[...], norm, scales[rows, 0:1]).astype(BF16)
        dz[rows, :] = d_z
        value = pre[rows, :]
        s = sigmoid(value)
        d_h = (mm_nt(d_z, w2[...]) * (s * (1.0 + value * (1.0 - s)))).astype(BF16)
        dh[rows, :] = d_h
        bias_sum = bias_sum + jnp.sum(d_h.astype(F32), axis=0, keepdims=True)
    vec[0:1, :] = bias_sum
    vec[1:2, :] = gain_sum
    r_vec = copies.remote(vec, vec_in.at[0], partner)
    spart[...] = mm(oht[...], dh[...])
    s_send[...] = spart[...].astype(BF16)
    r_s = copies.remote(s_send, s_in, partner)
    grad = mm_tn(edges[...], dh[...])
    for j in range(2):
        gfirst[j] = grad[:, j * hhalf : (j + 1) * hhalf]
    gfirst_send[...] = gfirst[other].astype(BF16)
    r_first = copies.remote(gfirst_send, first_in, partner)
    gsecond[...] = mm_tn(act[...], dz[...])
    gsecond_send[...] = gsecond[pl.ds(pl.multiple_of(other * hhalf, 128), hhalf), :].astype(BF16)
    r_second = copies.remote(gsecond_send, second_in, partner)

    node_red.take_half(0)
    node_red.send_half(1)

    r_s.wait()
    spart[...] = spart[...] + s_in[...].astype(F32)
    s_all = spart[...].astype(BF16)
    t_grad = mm_nt(s_all[:t_rows], w1[pl.ds(pl.multiple_of(width + h * half, 128), half), :])
    back[...] = t_grad[n_count:].astype(BF16)
    r_back_prev = copies.remote(
        back.at[pl.ds(0, halo)], arriving.at[pl.ds(halo, halo)], prev
    )
    r_back_next = copies.remote(
        back.at[pl.ds(halo, halo)], arriving.at[pl.ds(0, halo)], after
    )
    gnode[...] = (
        gnode[...]
        + t_grad[:n_count]
        + mm_nt(s_all[t_rows:], w1[pl.ds(pl.multiple_of(2 * width + h * half, 128), half), :])
    )
    s_mine = spart[:, my_hidden].astype(BF16)
    e_work[pl.ds(width, width), :] = mm_tn(table[...], s_mine[:t_rows]).astype(BF16)
    e_work[pl.ds(2 * width, width), :] = mm_tn(nodes[...], s_mine[t_rows:]).astype(BF16)
    r_first.wait()
    e_work[pl.ds(0, width), :] = (gfirst[h] + first_in[...].astype(F32)).astype(BF16)
    r_second.wait()
    grad = (gsecond[my_hidden, :] + second_in[...].astype(F32)).astype(BF16)
    for j in range(2):
        e_work[pl.ds(3 * width + j * hhalf, hhalf), :] = grad[:, j * half : (j + 1) * half]
    filled = 3 * width + 2 * hhalf
    if edge_rows_padded > filled:
        e_work[pl.ds(filled, edge_rows_padded - filled), :] = jnp.zeros(
            (edge_rows_padded - filled, half), BF16
        )
    edge_red = Reduction(copies, e_work, e_land, eg, edge_rows_padded, steps)
    edge_red.send_half(0)
    r_vec.wait()
    vec[...] = vec[...] + vec_in[0]

    for i in range(0, e_count, CHUNK):
        rows = pl.ds(i, CHUNK)
        own = (ecot[rows, :].astype(F32) + mm_nt(dh[rows, :], w1[:width, :])).astype(BF16)
        for j in range(2):
            ge_half[j, rows, :] = own[:, j * half : (j + 1) * half]
    r_ge = copies.remote(ge_half.at[other], ge_full.at[my_rows], partner)
    c_ge = copies.local(ge_half.at[h], ge_full.at[my_rows])
    r_back_prev.wait()
    r_back_next.wait()
    gnode[...] = gnode[...] + mm(pick_t, arriving[...])
    back_out = gnode[...].astype(BF16)
    outgoing[:, :half] = back_out
    c_gn = copies.local(outgoing.at[:, pl.ds(0, half)], gn_out)
    r_ge.wait()
    c_ge.wait()
    c_geo = copies.local(ge_full, ge_out)

    count = len(steps)
    r_vec = copies.remote(vec, vec_in.at[1], steps[0][0])
    for k in range(count):
        if k > 0:
            node_red.take_half(k)
            if k + 1 < count:
                node_red.send_half(k + 1)
            else:
                node_red.send_own(count - 1)
        edge_red.take_half(k)
        r_vec.wait()
        vec[...] = vec[...] + vec_in[k + 1]
        if k + 1 < count:
            edge_red.send_half(k + 1)
            r_vec = copies.remote(vec, vec_in.at[k + 2], steps[k + 1][0])
        else:
            edge_red.send_own(count - 1)
    c_vec = copies.local(vec, vec_out)
    for k in reversed(range(count)):
        node_red.take_own()
        if k > 0:
            node_red.send_own(k - 1)
        else:
            r_node = copies.remote(ng.at[h], ng.at[h], partner)
        edge_red.take_own()
        if k > 0:
            edge_red.send_own(k - 1)
    c_eg = copies.local(eg, eg_out)
    r_node.wait()
    c_ng = copies.local(ng, ng_out)
    for copy in (c_gn, c_geo, c_vec, c_eg, c_ng):
        copy.wait()


def on_device(
    mesh_sizes, nodes, edges, node_cotangent, edge_cotangent, senders, receivers, send_lists,
    edge_first, edge_bias, edge_second, edge_gain, node_first, node_bias, node_second, node_gain,
):
    batches, patches = mesh_sizes
    group = batches * patches
    n_count, width = nodes.shape[1:]
    e_all = edges.shape[1]
    e_count = e_all // 2
    hid = 2 * edge_second.shape[0]
    half, hhalf = width // 2, hid // 2
    halo = send_lists.shape[2]
    t_rows = n_count + 2 * halo
    unit = 16 * group
    n_rows = -(-(2 * width + 2 * hhalf) // unit) * unit
    e_rows = -(-(3 * width + 2 * hhalf) // unit) * unit
    part = lax.axis_index("hidden")
    steps = group.bit_length() - 1
    own_ids = lambda ids: lax.dynamic_slice_in_dim(ids, part * e_count, e_count, 0)[None]
    row = lambda vector: vector[None, :]
    bias_all = lax.all_gather(edge_bias, "hidden", axis=0, tiled=True)
    anywhere = pl.BlockSpec(memory_space=pl.ANY)
    inside = pl.BlockSpec(memory_space=pltpu.VMEM)
    V = pltpu.VMEM
    outs = pl.pallas_call(
        functools.partial(kernel, (batches, patches, n_rows, e_rows)),
        out_shape=(
            jax.ShapeDtypeStruct((n_count, half), BF16),
            jax.ShapeDtypeStruct((e_all, half), BF16),
            jax.ShapeDtypeStruct((2, n_rows, half), BF16),
            jax.ShapeDtypeStruct((e_rows, half), BF16),
            jax.ShapeDtypeStruct((8, width), F32),
        ),
        in_specs=[
            anywhere, anywhere, anywhere, anywhere, inside, inside, inside,
            anywhere, inside, anywhere, inside, anywhere, inside, anywhere, inside,
        ],
        out_specs=(anywhere,) * 5,
        scratch_shapes=[
            V((n_count, width), BF16),
            V((e_count, width), BF16),
            V((n_count, width), BF16),
            V((e_count, width), BF16),
            V((3 * width, hid), BF16),
            V((hid, width), BF16),
            V((2 * width, hid), BF16),
            V((hid, width), BF16),
            V((t_rows, width), BF16),
            V((2 * halo, width), BF16),
            V((t_rows + n_count, e_count), BF16),
            V((e_count, t_rows + n_count), BF16),
            V((e_count, hid), F32),
            V((e_count, hid), BF16),
            V((e_count, width), F32),
            V((e_count, 128), F32),
            V((e_count, width), BF16),
            V((2, n_count, width), F32),
            V((2, n_count, width), BF16),
            V((n_count, hid), BF16),
            V((e_count, width), BF16),
            V((e_count, hid), BF16),
            V((2, width, hhalf), F32),
            V((width, hhalf), BF16),
            V((hid, width), F32),
            V((hhalf, width), BF16),
            V((width, hhalf), BF16),
            V((hhalf, width), BF16),
            V((t_rows + n_count, hid), F32),
            V((t_rows + n_count, hid), BF16),
            V((t_rows + n_count, hid), BF16),
            V((2, e_count, half), BF16),
            V((e_all, half), BF16),
            V((2 * halo, half), BF16),
            V((2 * halo, half), BF16),
            V((n_count, half), F32),
            V((2, n_rows, half), BF16),
            V((n_rows, half), BF16),
            V((n_rows, half), BF16),
            V((e_rows, half), BF16),
            V((e_rows, half), BF16),
            V((e_rows, half), BF16),
            V((8, width), F32),
            V((steps + 1, 8, width), F32),
            pltpu.SemaphoreType.DMA((16,)),
            pltpu.SemaphoreType.DMA((16 + 5 * steps,)),
            pltpu.SemaphoreType.DMA((16 + 5 * steps,)),
        ],
        compiler_params=pltpu.CompilerParams(
            collective_id=0, has_side_effects=True, vmem_limit_bytes=60 * 1024 * 1024
        ),
    )(
        nodes[0], edges[0], node_cotangent[0], edge_cotangent[0],
        own_ids(senders), own_ids(receivers), send_lists.reshape(1, -1),
        edge_first, row(bias_all), edge_second, row(edge_gain),
        node_first, row(node_bias), node_second, row(node_gain),
    )
    g_nodes, g_edges, g_node, g_edge, vec = outs
    side = lambda rows: jnp.concatenate(jnp.split(rows, 2, axis=0), axis=1)
    g_node_first = jnp.concatenate([side(g_node[j, : 2 * width]) for j in range(2)], axis=0)
    g_node_second = jnp.concatenate(
        [side(g_node[j, 2 * width : 2 * width + 2 * hhalf]) for j in range(2)], axis=0
    )
    return (
        g_nodes[None],
        g_edges[None],
        g_edge[: 3 * width].astype(F32),
        lax.dynamic_slice_in_dim(vec[0], part * hhalf, hhalf, 0),
        side(g_edge[3 * width : 3 * width + 2 * hhalf]).astype(F32),
        vec[1],
        g_node_first.astype(F32),
        vec[2],
        g_node_second.astype(F32),
        vec[3],
    )


def solution(mesh):
    placed = (
        P("batch", "space", None), P("batch", "space", None),
        P("batch", "space", None), P("batch", "space", None),
        P("space"), P("space"), P("space", None, None),
        P(None, "hidden"), P("hidden"), P("hidden", None),
        P(), P(), P(), P(), P(),
    )
    batches, patches = mesh.shape["batch"], mesh.shape["space"]
    assert mesh.shape["hidden"] == 2 and batches == 2
    assert patches & (patches - 1) == 0
    return jax.shard_map(
        functools.partial(on_device, (batches, patches)),
        mesh=mesh,
        in_specs=placed,
        out_specs=(
            P("batch", "space", "hidden"), P("batch", "space", "hidden"),
            P(None, "hidden"), P("hidden"), P("hidden", None),
            P(), P(), P(), P(), P(),
        ),
        check_vma=False,
    )
```

```python
import functools

import jax
import jax.numpy as jnp
from jax import lax
from jax.experimental import pallas as pl
from jax.experimental.pallas import tpu as pltpu
from jax.sharding import PartitionSpec as P

EPS = 1e-05
CHUNK = 256
F32, BF16 = jnp.float32, jnp.bfloat16
MESH = pl.DeviceIdType.MESH


def mm(lefthand, righthand):
    return jnp.dot(lefthand, righthand, preferred_element_type=F32)


def mm_tn(lefthand, righthand):
    return lax.dot_general(
        lefthand, righthand, (((0,), (0,)), ((), ())), preferred_element_type=F32
    )


def mm_nt(lefthand, righthand):
    return lax.dot_general(
        lefthand, righthand, (((1,), (1,)), ((), ())), preferred_element_type=F32
    )


def normalize(values):
    centre = values - jnp.mean(values, axis=-1, keepdims=True)
    scaled = lax.rsqrt(jnp.mean(centre * centre, axis=-1, keepdims=True) + EPS)
    return centre * scaled, scaled


def norm_back(upstream, gain, normed, scaled):
    pulled = upstream * gain
    return scaled * (
        pulled
        - jnp.mean(pulled, axis=-1, keepdims=True)
        - normed * jnp.mean(pulled * normed, axis=-1, keepdims=True)
    )


def sigmoid(values):
    return 1.0 / (1.0 + jnp.exp(-values))


class Copies:
    def __init__(self, local_sems, send_sems, recv_sems):
        self.local_sems, self.send_sems, self.recv_sems = local_sems, send_sems, recv_sems
        self.locals, self.remotes = 0, 0

    def local(self, src, dst):
        copy = pltpu.make_async_copy(src, dst, self.local_sems.at[self.locals])
        self.locals += 1
        copy.start()
        return copy

    def remote(self, src, dst, device):
        copy = pltpu.make_async_remote_copy(
            src_ref=src,
            dst_ref=dst,
            send_sem=self.send_sems.at[self.remotes],
            recv_sem=self.recv_sems.at[self.remotes],
            device_id=device,
            device_id_type=MESH,
        )
        self.remotes += 1
        copy.start()
        return copy


class Reduction:
    def __init__(self, copies, buf, landing, result, rows, steps):
        self.copies, self.buf, self.landing, self.result = copies, buf, landing, result
        self.steps = steps
        self.size = rows
        self.offset = 0
        self.land = 0
        self.trail = []
        self.flight = None
        self.stage = 0
        self.done = False

    def _rows(self, start, size):
        return pl.ds(pl.multiple_of(start, 16), size)

    def send_half(self, index):
        device, bit = self.steps[index]
        half = self.size // 2
        theirs = self.offset + (1 - bit) * half
        self.flight = self.copies.remote(
            self.buf.at[self._rows(theirs, half)],
            self.landing.at[pl.ds(self.land, half)],
            device,
        )

    def take_half(self, index):
        device, bit = self.steps[index]
        half = self.size // 2
        self.flight.wait()
        mine = self.offset + bit * half
        block = 64
        while half % block:
            block //= 2
        land = self.land
        target = self.result if index + 1 == len(self.steps) else self.buf

        def add(i, carry):
            here = pl.ds(pl.multiple_of(mine + i * block, 16), block)
            there = pl.ds(pl.multiple_of(land + i * block, 16), block)
            target[here, :] = (
                self.buf[here, :].astype(F32) + self.landing[there, :].astype(F32)
            ).astype(BF16)
            return carry

        lax.fori_loop(0, half // block, add, 0)
        self.trail.append((self.offset, self.size))
        self.offset, self.size, self.land = mine, half, land + half
        self.stage += 1

    def advance(self):
        count = len(self.steps)
        if self.done:
            return
        if self.stage < count:
            self.take_half(self.stage)
            if self.stage < count:
                self.send_half(self.stage)
            else:
                self.send_own(count - 1)
        else:
            self.take_own()
            if self.stage < 2 * count:
                self.send_own(2 * count - 1 - self.stage)
            else:
                self.done = True

    def send_own(self, index):
        device, _ = self.steps[index]
        rows = self._rows(self.offset, self.size)
        self.flight = self.copies.remote(self.result.at[rows], self.result.at[rows], device)

    def take_own(self):
        self.flight.wait()
        self.offset, self.size = self.trail.pop()
        self.stage += 1


def kernel(
    sizes,
    nodes_h, edges_h, ncot_h, ecot_h, senders_v, receivers_v, lists_v,
    first_h, ebias_v, second_h, egain_v, nfirst_h, nbias_v, nsecond_h, ngain_v,
    gn_out, ge_out, ng_out, eg_out, vec_out,
    nodes, edges, ncot, ecot, w1, w2, n1, n2,
    table, outgoing, oht, oh, pre, act, normed, scales, msg, agg, nin, nact, dz, dh,
    gfirst, gfirst_send, gsecond, gsecond_send, first_in, second_in,
    spart, s_send, s_in, ge_half, ge_full, back, arriving, gnode,
    ng, n_work, n_land, eg, top, top_land, low, low_land, vec, vec_in, bias,
    local_sems, send_sems, recv_sems,
):
    batches, patches, node_rows_padded, edge_rows_padded = sizes
    b, p, h = lax.axis_index("batch"), lax.axis_index("space"), lax.axis_index("hidden")
    other = 1 - h
    partner = (b, p, other)
    prev = (b, lax.rem(p + patches - 1, patches), h)
    after = (b, lax.rem(p + 1, patches), h)
    n_count, width = nodes.shape
    e_count = edges.shape[0]
    half = width // 2
    halo = lists_v.shape[1]
    t_rows = table.shape[0]
    hid = w2.shape[0]
    hhalf = hid // 2

    def flip_space(bit_index):
        stride = 1 << bit_index
        bit = lax.rem(p // stride, 2)
        return (b, p + stride * (1 - 2 * bit), h), bit

    def flip_batch():
        return (1 - b, p, h), b

    bits = patches.bit_length() - 1
    rest = [flip_space(i) for i in range(1, bits)]
    near, far = flip_space(0), flip_batch()
    pn = p + (1 - 2 * lax.rem(p, 2))
    one = ((b * (1 - h) + (1 - b) * h, pn * (1 - h) + p * h, h), near[1] * (1 - h) + far[1] * h)
    two = (((1 - b) * (1 - h) + b * h, p * (1 - h) + pn * h, h), far[1] * (1 - h) + near[1] * h)
    steps = [one, two] + rest

    def clear(ref, filled):
        if ref.shape[0] > filled:
            ref[pl.ds(filled, ref.shape[0] - filled), :] = jnp.zeros(
                (ref.shape[0] - filled, half), BF16
            )

    copies = Copies(local_sems, send_sems, recv_sems)
    my_rows = pl.ds(pl.multiple_of(h * e_count, 128), e_count)
    my_hidden = pl.ds(pl.multiple_of(h * hhalf, 128), hhalf)
    c_nodes = copies.local(nodes_h, nodes)
    c_w1 = copies.local(first_h, w1.at[:, my_hidden])
    c_edges = copies.local(edges_h.at[my_rows], edges)
    c_w2 = copies.local(second_h, w2.at[my_hidden])
    c_n1 = copies.local(nfirst_h, n1)
    c_n2 = copies.local(nsecond_h, n2)
    c_ncot = copies.local(ncot_h, ncot)
    c_ecot = copies.local(ecot_h.at[my_rows], ecot)

    barrier = pltpu.get_barrier_semaphore()
    friends = [partner, prev, after] + [device for device, _ in steps]
    for device in friends:
        pl.semaphore_signal(barrier, inc=1, device_id=device, device_id_type=MESH)
    c_nodes.wait()
    lines = lax.broadcasted_iota(jnp.int32, (n_count, halo), 0)
    pick_t = [(lines == lists_v[j : j + 1, :]).astype(BF16) for j in range(2)]
    for j in range(2):
        outgoing[pl.ds(j * halo, halo), :] = mm_tn(pick_t[j], nodes[...]).astype(BF16)
    pl.semaphore_wait(barrier, len(friends))
    r_bias = copies.remote(ebias_v, bias.at[:, my_hidden], partner)
    bias[:, my_hidden] = ebias_v[...]
    r_w1 = copies.remote(first_h, w1.at[:, my_hidden], partner)
    r_w2 = copies.remote(second_h, w2.at[my_hidden], partner)
    r_prev = copies.remote(
        outgoing.at[pl.ds(0, halo)], table.at[pl.ds(n_count + halo, halo)], prev
    )
    r_next = copies.remote(outgoing.at[pl.ds(halo, halo)], table.at[pl.ds(n_count, halo)], after)
    table[pl.ds(0, n_count), :] = nodes[...]
    oht[pl.ds(0, t_rows), :] = (
        lax.broadcasted_iota(jnp.int32, (t_rows, e_count), 0) == senders_v[:, my_rows]
    ).astype(BF16)
    oht[pl.ds(t_rows, n_count), :] = (
        lax.broadcasted_iota(jnp.int32, (n_count, e_count), 0) == receivers_v[:, my_rows]
    ).astype(BF16)
    oh[...] = oht[...].astype(F32).T.astype(BF16)

    c_w1.wait()
    c_w2.wait()
    r_w1.wait()
    r_bias.wait()
    p_recv = mm(nodes[...], w1[2 * width :, :]).astype(BF16)
    c_edges.wait()
    for i in range(0, e_count, CHUNK):
        rows = pl.ds(i, CHUNK)
        pre[rows, :] = (
            mm(edges[rows, :], w1[:width, :]) + mm(oh[rows, t_rows:], p_recv) + bias[...]
        )
    r_prev.wait()
    r_next.wait()
    r_w2.wait()
    p_send = mm(table[...], w1[width : 2 * width, :]).astype(BF16)
    for i in range(0, e_count, CHUNK):
        rows = pl.ds(i, CHUNK)
        value = pre[rows, :] + mm(oh[rows, :t_rows], p_send)
        pre[rows, :] = value
        active = (value * sigmoid(value)).astype(BF16)
        act[rows, :] = active
        norm, scale = normalize(mm(active, w2[...]))
        normed[rows, :] = norm
        scales[rows, :] = jnp.broadcast_to(scale, (CHUNK, 128))
        msg[rows, :] = (egain_v[...] * norm).astype(BF16)
    agg[0] = mm(oht[t_rows:, :], msg[...])
    r_agg = copies.remote(agg.at[0], agg.at[1], partner)
    c_n1.wait()
    c_n2.wait()
    c_ncot.wait()
    node_half = mm(nodes[...], n1[:width, :]) + nbias_v[...]
    nin[0] = nodes[...]
    r_agg.wait()
    gathered = (agg[0] + agg[1]).astype(BF16)
    nin[1] = gathered

    n_pre = node_half + mm(gathered, n1[width:, :])
    n_sig = sigmoid(n_pre)
    n_active = (n_pre * n_sig).astype(BF16)
    nact[...] = n_active
    n_norm, n_scale = normalize(mm(n_active, n2[...]))
    n_up = ncot[...].astype(F32)
    first_core = (1 - h).astype(F32)
    vec[...] = jnp.zeros_like(vec)
    vec[3:4, :] = jnp.sum(n_up * n_norm, axis=0, keepdims=True) * first_core
    n_dz = norm_back(n_up, ngain_v[...], n_norm, n_scale).astype(BF16)
    n_slope = n_sig * (1.0 + n_pre * (1.0 - n_sig))
    n_dh = (mm_nt(n_dz, n2[...]) * n_slope).astype(BF16)
    vec[2:3, :] = jnp.sum(n_dh.astype(F32), axis=0, keepdims=True) * first_core
    agg_grad = mm_nt(n_dh, n1[width:, :]).astype(BF16)
    my_feat = pl.ds(pl.multiple_of(h * half, 128), half)
    gnode[...] = ncot[:, my_feat].astype(F32) + mm_nt(n_dh, n1[my_feat, :])
    ngh = n_work
    grad = mm_tn(nin[h], n_dh).astype(BF16)
    for j in range(2):
        ngh[pl.ds(j * width, width), :] = grad[:, j * half : (j + 1) * half]
    grad = mm_tn(nact[:, my_hidden], n_dz).astype(BF16)
    for j in range(2):
        ngh[pl.ds(2 * width + j * hhalf, hhalf), :] = grad[:, j * half : (j + 1) * half]
    clear(ngh, 2 * width + 2 * hhalf)
    node_red = Reduction(copies, n_work, n_land, ng.at[h], node_rows_padded, steps)
    node_red.send_half(0)

    c_ecot.wait()
    gain_sum = jnp.zeros((1, width), F32)
    bias_sum = jnp.zeros((1, hid), F32)
    for i in range(0, e_count, CHUNK):
        rows = pl.ds(i, CHUNK)
        upstream = ecot[rows, :].astype(F32)
        norm = normed[rows, :]
        grad = upstream + mm(oh[rows, t_rows:], agg_grad)
        gain_sum = gain_sum + jnp.sum(grad * norm, axis=0, keepdims=True)
        d_z = norm_back(grad, egain_v[...], norm, scales[rows, 0:1]).astype(BF16)
        dz[rows, :] = d_z
        value = pre[rows, :]
        s = sigmoid(value)
        d_h = (mm_nt(d_z, w2[...]) * (s * (1.0 + value * (1.0 - s)))).astype(BF16)
        dh[rows, :] = d_h
        bias_sum = bias_sum + jnp.sum(d_h.astype(F32), axis=0, keepdims=True)
    vec[0:1, :] = bias_sum
    vec[1:2, :] = gain_sum
    r_vec = copies.remote(vec, vec_in.at[0], partner)
    grad = mm_tn(edges[...], dh[...])
    for j in range(2):
        gfirst[j] = grad[:, j * hhalf : (j + 1) * hhalf]
    gfirst_send[...] = gfirst[other].astype(BF16)
    r_first = copies.remote(gfirst_send, first_in, partner)
    gsecond[...] = mm_tn(act[...], dz[...])
    gsecond_send[...] = gsecond[pl.ds(pl.multiple_of(other * hhalf, 128), hhalf), :].astype(BF16)
    r_second = copies.remote(gsecond_send, second_in, partner)
    spart[...] = mm(oht[...], dh[...])
    s_send[...] = spart[...].astype(BF16)
    r_s = copies.remote(s_send, s_in, partner)
    node_red.advance()
    r_first.wait()
    top[pl.ds(0, width), :] = (gfirst[h] + first_in[...].astype(F32)).astype(BF16)
    r_second.wait()
    grad = (gsecond[my_hidden, :] + second_in[...].astype(F32)).astype(BF16)
    for j in range(2):
        top[pl.ds(width + j * hhalf, hhalf), :] = grad[:, j * half : (j + 1) * half]
    clear(top, width + 2 * hhalf)
    top_red = Reduction(copies, top, top_land, eg.at[0], edge_rows_padded, steps)
    top_red.send_half(0)
    node_red.advance()

    r_s.wait()
    spart[...] = spart[...] + s_in[...].astype(F32)
    s_all = spart[...].astype(BF16)
    t_grad = mm_nt(s_all[:t_rows], w1[pl.ds(pl.multiple_of(width + h * half, 128), half), :])
    back[...] = t_grad[n_count:].astype(BF16)
    r_back_prev = copies.remote(
        back.at[pl.ds(0, halo)], arriving.at[pl.ds(halo, halo)], prev
    )
    r_back_next = copies.remote(
        back.at[pl.ds(halo, halo)], arriving.at[pl.ds(0, halo)], after
    )
    gnode[...] = (
        gnode[...]
        + t_grad[:n_count]
        + mm_nt(s_all[t_rows:], w1[pl.ds(pl.multiple_of(2 * width + h * half, 128), half), :])
    )
    s_mine = spart[:, my_hidden].astype(BF16)
    low[pl.ds(0, width), :] = mm_tn(table[...], s_mine[:t_rows]).astype(BF16)
    low[pl.ds(width, width), :] = mm_tn(nodes[...], s_mine[t_rows:]).astype(BF16)
    clear(low, 2 * width)
    low_red = Reduction(copies, low, low_land, eg.at[1], edge_rows_padded, steps)
    low_red.send_half(0)
    node_red.advance()
    r_vec.wait()
    vec[...] = vec[...] + vec_in[0]
    count = len(steps)
    r_node = None

    for i in range(0, e_count, CHUNK):
        rows = pl.ds(i, CHUNK)
        own = (ecot[rows, :].astype(F32) + mm_nt(dh[rows, :], w1[:width, :])).astype(BF16)
        for j in range(2):
            ge_half[j, rows, :] = own[:, j * half : (j + 1) * half]
    r_ge = copies.remote(ge_half.at[other], ge_full.at[my_rows], partner)
    c_ge = copies.local(ge_half.at[h], ge_full.at[my_rows])
    r_back_prev.wait()
    r_back_next.wait()
    gnode[...] = gnode[...] + (
        mm(pick_t[0], arriving[:halo]) + mm(pick_t[1], arriving[halo:])
    )
    back_out = gnode[...].astype(BF16)
    outgoing[:, :half] = back_out
    c_gn = copies.local(outgoing.at[:, pl.ds(0, half)], gn_out)
    r_ge.wait()
    c_ge.wait()
    c_geo = copies.local(ge_full, ge_out)

    r_vec = copies.remote(vec, vec_in.at[1], steps[0][0])
    top_red.advance()
    low_red.advance()
    for k in range(count):
        r_vec.wait()
        vec[...] = vec[...] + vec_in[k + 1]
        if k + 1 < count:
            r_vec = copies.remote(vec, vec_in.at[k + 2], steps[k + 1][0])
        node_red.advance()
        top_red.advance()
        low_red.advance()
    c_vec = copies.local(vec, vec_out)
    while not (node_red.done and top_red.done and low_red.done):
        node_red.advance()
        if node_red.done and r_node is None:
            r_node = copies.remote(ng.at[h], ng.at[h], partner)
        top_red.advance()
        low_red.advance()
    c_eg = copies.local(eg, eg_out)
    r_node.wait()
    c_ng = copies.local(ng, ng_out)
    for copy in (c_gn, c_geo, c_vec, c_eg, c_ng):
        copy.wait()


def on_device(
    mesh_sizes, nodes, edges, node_cotangent, edge_cotangent, senders, receivers, send_lists,
    edge_first, edge_bias, edge_second, edge_gain, node_first, node_bias, node_second, node_gain,
):
    batches, patches = mesh_sizes
    group = batches * patches
    n_count, width = nodes.shape[1:]
    e_all = edges.shape[1]
    e_count = e_all // 2
    hid = 2 * edge_second.shape[0]
    half, hhalf = width // 2, hid // 2
    halo = send_lists.shape[2]
    t_rows = n_count + 2 * halo
    unit = 16 * group
    n_rows = -(-(2 * width + 2 * hhalf) // unit) * unit
    e_rows = -(-max(2 * width, width + 2 * hhalf) // unit) * unit
    part = lax.axis_index("hidden")
    steps = group.bit_length() - 1
    row = lambda vector: vector[None, :]
    anywhere = pl.BlockSpec(memory_space=pl.ANY)
    inside = pl.BlockSpec(memory_space=pltpu.VMEM)
    V = pltpu.VMEM
    outs = pl.pallas_call(
        functools.partial(kernel, (batches, patches, n_rows, e_rows)),
        out_shape=(
            jax.ShapeDtypeStruct((n_count, half), BF16),
            jax.ShapeDtypeStruct((e_all, half), BF16),
            jax.ShapeDtypeStruct((2, n_rows, half), BF16),
            jax.ShapeDtypeStruct((2, e_rows, half), BF16),
            jax.ShapeDtypeStruct((8, width), F32),
        ),
        in_specs=[
            anywhere, anywhere, anywhere, anywhere, inside, inside, inside,
            anywhere, inside, anywhere, inside, anywhere, inside, anywhere, inside,
        ],
        out_specs=(anywhere,) * 5,
        scratch_shapes=[
            V((n_count, width), BF16),
            V((e_count, width), BF16),
            V((n_count, width), BF16),
            V((e_count, width), BF16),
            V((3 * width, hid), BF16),
            V((hid, width), BF16),
            V((2 * width, hid), BF16),
            V((hid, width), BF16),
            V((t_rows, width), BF16),
            V((2 * halo, width), BF16),
            V((t_rows + n_count, e_count), BF16),
            V((e_count, t_rows + n_count), BF16),
            V((e_count, hid), F32),
            V((e_count, hid), BF16),
            V((e_count, width), F32),
            V((e_count, 128), F32),
            V((e_count, width), BF16),
            V((2, n_count, width), F32),
            V((2, n_count, width), BF16),
            V((n_count, hid), BF16),
            V((e_count, width), BF16),
            V((e_count, hid), BF16),
            V((2, width, hhalf), F32),
            V((width, hhalf), BF16),
            V((hid, width), F32),
            V((hhalf, width), BF16),
            V((width, hhalf), BF16),
            V((hhalf, width), BF16),
            V((t_rows + n_count, hid), F32),
            V((t_rows + n_count, hid), BF16),
            V((t_rows + n_count, hid), BF16),
            V((2, e_count, half), BF16),
            V((e_all, half), BF16),
            V((2 * halo, half), BF16),
            V((2 * halo, half), BF16),
            V((n_count, half), F32),
            V((2, n_rows, half), BF16),
            V((n_rows, half), BF16),
            V((n_rows, half), BF16),
            V((2, e_rows, half), BF16),
            V((e_rows, half), BF16),
            V((e_rows, half), BF16),
            V((e_rows, half), BF16),
            V((e_rows, half), BF16),
            V((8, width), F32),
            V((steps + 1, 8, width), F32),
            V((1, hid), F32),
            pltpu.SemaphoreType.DMA((16,)),
            pltpu.SemaphoreType.DMA((16 + 7 * steps,)),
            pltpu.SemaphoreType.DMA((16 + 7 * steps,)),
        ],
        compiler_params=pltpu.CompilerParams(
            collective_id=0, has_side_effects=True, vmem_limit_bytes=60 * 1024 * 1024
        ),
    )(
        nodes[0], edges[0], node_cotangent[0], edge_cotangent[0],
        row(senders), row(receivers), send_lists[0],
        edge_first, row(edge_bias), edge_second, row(edge_gain),
        node_first, row(node_bias), node_second, row(node_gain),
    )
    g_nodes, g_edges, g_node, g_edge, vec = outs
    side = lambda rows: jnp.concatenate(jnp.split(rows, 2, axis=0), axis=1)
    g_node_first = jnp.concatenate([side(g_node[j, : 2 * width]) for j in range(2)], axis=0)
    g_node_second = jnp.concatenate(
        [side(g_node[j, 2 * width : 2 * width + 2 * hhalf]) for j in range(2)], axis=0
    )
    return (
        g_nodes[None],
        g_edges[None],
        jnp.concatenate([g_edge[0, :width], g_edge[1, : 2 * width]], axis=0).astype(F32),
        lax.dynamic_slice_in_dim(vec[0], part * hhalf, hhalf, 0),
        side(g_edge[0, width : width + 2 * hhalf]).astype(F32),
        vec[1],
        g_node_first.astype(F32),
        vec[2],
        g_node_second.astype(F32),
        vec[3],
    )


def solution(mesh):
    placed = (
        P("batch", "space", None), P("batch", "space", None),
        P("batch", "space", None), P("batch", "space", None),
        P("space"), P("space"), P("space", None, None),
        P(None, "hidden"), P("hidden"), P("hidden", None),
        P(), P(), P(), P(), P(),
    )
    batches, patches = mesh.shape["batch"], mesh.shape["space"]
    assert mesh.shape["hidden"] == 2 and batches == 2
    assert patches & (patches - 1) == 0
    return jax.shard_map(
        functools.partial(on_device, (batches, patches)),
        mesh=mesh,
        in_specs=placed,
        out_specs=(
            P("batch", "space", "hidden"), P("batch", "space", "hidden"),
            P(None, "hidden"), P("hidden"), P("hidden", None),
            P(), P(), P(), P(), P(),
        ),
        check_vma=False,
    )
```

```python
import functools

import jax
import jax.numpy as jnp
from jax import lax
from jax.experimental import pallas as pl
from jax.experimental.pallas import tpu as pltpu
from jax.sharding import PartitionSpec as P

EPS = 1e-05
CHUNK = 256
F32, BF16 = jnp.float32, jnp.bfloat16
MESH = pl.DeviceIdType.MESH


def mm(lefthand, righthand):
    return jnp.dot(lefthand, righthand, preferred_element_type=F32)


def mm_tn(lefthand, righthand):
    return lax.dot_general(
        lefthand, righthand, (((0,), (0,)), ((), ())), preferred_element_type=F32
    )


def mm_nt(lefthand, righthand):
    return lax.dot_general(
        lefthand, righthand, (((1,), (1,)), ((), ())), preferred_element_type=F32
    )


def normalize(values):
    centre = values - jnp.mean(values, axis=-1, keepdims=True)
    scaled = lax.rsqrt(jnp.mean(centre * centre, axis=-1, keepdims=True) + EPS)
    return centre * scaled, scaled


def norm_back(upstream, gain, normed, scaled):
    pulled = upstream * gain
    return scaled * (
        pulled
        - jnp.mean(pulled, axis=-1, keepdims=True)
        - normed * jnp.mean(pulled * normed, axis=-1, keepdims=True)
    )


def sigmoid(values):
    return 1.0 / (1.0 + jnp.exp(-values))


class Copies:
    def __init__(self, local_sems, send_sems, recv_sems):
        self.local_sems, self.send_sems, self.recv_sems = local_sems, send_sems, recv_sems
        self.locals, self.remotes = 0, 0

    def local(self, src, dst):
        copy = pltpu.make_async_copy(src, dst, self.local_sems.at[self.locals])
        self.locals += 1
        copy.start()
        return copy

    def remote(self, src, dst, device):
        copy = pltpu.make_async_remote_copy(
            src_ref=src,
            dst_ref=dst,
            send_sem=self.send_sems.at[self.remotes],
            recv_sem=self.recv_sems.at[self.remotes],
            device_id=device,
            device_id_type=MESH,
        )
        self.remotes += 1
        copy.start()
        return copy


class Reduction:
    def __init__(self, copies, buf, landing, result, rows, steps):
        self.copies, self.buf, self.landing, self.result = copies, buf, landing, result
        self.steps = steps
        self.size = rows
        self.offset = 0
        self.land = 0
        self.trail = []
        self.flight = None
        self.stage = 0
        self.done = False

    def _rows(self, start, size):
        return pl.ds(pl.multiple_of(start, 16), size)

    def send_half(self, index):
        device, bit = self.steps[index]
        half = self.size // 2
        theirs = self.offset + (1 - bit) * half
        self.flight = self.copies.remote(
            self.buf.at[self._rows(theirs, half)],
            self.landing.at[pl.ds(self.land, half)],
            device,
        )

    def take_half(self, index):
        device, bit = self.steps[index]
        half = self.size // 2
        self.flight.wait()
        mine = self.offset + bit * half
        block = 64
        while half % block:
            block //= 2
        land = self.land
        target = self.result if index + 1 == len(self.steps) else self.buf

        def add(i, carry):
            here = pl.ds(pl.multiple_of(mine + i * block, 16), block)
            there = pl.ds(pl.multiple_of(land + i * block, 16), block)
            target[here, :] = (
                self.buf[here, :].astype(F32) + self.landing[there, :].astype(F32)
            ).astype(BF16)
            return carry

        lax.fori_loop(0, half // block, add, 0)
        self.trail.append((self.offset, self.size))
        self.offset, self.size, self.land = mine, half, land + half
        self.stage += 1

    def advance(self):
        count = len(self.steps)
        if self.done:
            return
        if self.stage < count:
            self.take_half(self.stage)
            if self.stage < count:
                self.send_half(self.stage)
            else:
                self.send_own(count - 1)
        else:
            self.take_own()
            if self.stage < 2 * count:
                self.send_own(2 * count - 1 - self.stage)
            else:
                self.done = True

    def send_own(self, index):
        device, _ = self.steps[index]
        rows = self._rows(self.offset, self.size)
        self.flight = self.copies.remote(self.result.at[rows], self.result.at[rows], device)

    def take_own(self):
        self.flight.wait()
        self.offset, self.size = self.trail.pop()
        self.stage += 1


def kernel(
    sizes,
    nodes_h, edges_h, ncot_h, ecot_h, senders_v, receivers_v, lists_v,
    first_h, ebias_v, second_h, egain_v, nfirst_h, nbias_v, nsecond_h, ngain_v,
    gn_out, ge_out, ef_out, es_out, nf_out, ns_out, vec_out,
    nodes, edges, ncot, ecot, w1, w2, n1, n2,
    table, outgoing, oht, oh, pre, act, normed, scales, msg, agg, nin, nact, dz, dh,
    gfirst, gfirst_send, gsecond, gsecond_send, first_in, second_in,
    spart, s_send, s_in, ge_half, ge_full, back, arriving, gnode,
    ng, n_work, n_land, eg, top, top_land, low, low_land, vec, vec_in, bias,
    local_sems, send_sems, recv_sems,
):
    batches, patches, node_rows_padded, edge_rows_padded = sizes
    b, p, h = lax.axis_index("batch"), lax.axis_index("space"), lax.axis_index("hidden")
    other = 1 - h
    partner = (b, p, other)
    prev = (b, lax.rem(p + patches - 1, patches), h)
    after = (b, lax.rem(p + 1, patches), h)
    n_count, width = nodes.shape
    e_count = edges.shape[0]
    half = width // 2
    halo = lists_v.shape[1]
    t_rows = table.shape[0]
    hid = w2.shape[0]
    hhalf = hid // 2

    def flip_space(bit_index):
        stride = 1 << bit_index
        bit = lax.rem(p // stride, 2)
        return (b, p + stride * (1 - 2 * bit), h), bit

    def flip_batch():
        return (1 - b, p, h), b

    bits = patches.bit_length() - 1
    rest = [flip_space(i) for i in range(1, bits)]
    near, far = flip_space(0), flip_batch()
    pn = p + (1 - 2 * lax.rem(p, 2))
    one = ((b * (1 - h) + (1 - b) * h, pn * (1 - h) + p * h, h), near[1] * (1 - h) + far[1] * h)
    two = (((1 - b) * (1 - h) + b * h, p * (1 - h) + pn * h, h), far[1] * (1 - h) + near[1] * h)
    steps = [one, two] + rest

    def clear(ref, filled):
        if ref.shape[0] > filled:
            ref[pl.ds(filled, ref.shape[0] - filled), :] = jnp.zeros(
                (ref.shape[0] - filled, half), BF16
            )

    copies = Copies(local_sems, send_sems, recv_sems)
    my_rows = pl.ds(pl.multiple_of(h * e_count, 128), e_count)
    my_hidden = pl.ds(pl.multiple_of(h * hhalf, 128), hhalf)
    c_nodes = copies.local(nodes_h, nodes)
    c_w1 = copies.local(first_h, w1.at[:, my_hidden])
    c_edges = copies.local(edges_h.at[my_rows], edges)
    c_w2 = copies.local(second_h, w2.at[my_hidden])
    c_n1 = copies.local(nfirst_h, n1)
    c_n2 = copies.local(nsecond_h, n2)
    c_ncot = copies.local(ncot_h, ncot)
    c_ecot = copies.local(ecot_h.at[my_rows], ecot)

    barrier = pltpu.get_barrier_semaphore()
    friends = [partner, prev, after] + [device for device, _ in steps]
    for device in friends:
        pl.semaphore_signal(barrier, inc=1, device_id=device, device_id_type=MESH)
    c_nodes.wait()
    lines = lax.broadcasted_iota(jnp.int32, (n_count, halo), 0)
    pick_t = [(lines == lists_v[j : j + 1, :]).astype(BF16) for j in range(2)]
    for j in range(2):
        outgoing[pl.ds(j * halo, halo), :] = mm_tn(pick_t[j], nodes[...]).astype(BF16)
    pl.semaphore_wait(barrier, len(friends))
    r_bias = copies.remote(ebias_v, bias.at[:, my_hidden], partner)
    bias[:, my_hidden] = ebias_v[...]
    r_w1 = copies.remote(first_h, w1.at[:, my_hidden], partner)
    r_w2 = copies.remote(second_h, w2.at[my_hidden], partner)
    r_prev = copies.remote(
        outgoing.at[pl.ds(0, halo)], table.at[pl.ds(n_count + halo, halo)], prev
    )
    r_next = copies.remote(outgoing.at[pl.ds(halo, halo)], table.at[pl.ds(n_count, halo)], after)
    table[pl.ds(0, n_count), :] = nodes[...]
    oht[pl.ds(0, t_rows), :] = (
        lax.broadcasted_iota(jnp.int32, (t_rows, e_count), 0) == senders_v[:, my_rows]
    ).astype(BF16)
    oht[pl.ds(t_rows, n_count), :] = (
        lax.broadcasted_iota(jnp.int32, (n_count, e_count), 0) == receivers_v[:, my_rows]
    ).astype(BF16)
    oh[...] = oht[...].astype(F32).T.astype(BF16)

    c_w1.wait()
    c_w2.wait()
    r_w1.wait()
    r_bias.wait()
    p_recv = mm(nodes[...], w1[2 * width :, :]).astype(BF16)
    c_edges.wait()
    for i in range(0, e_count, CHUNK):
        rows = pl.ds(i, CHUNK)
        pre[rows, :] = (
            mm(edges[rows, :], w1[:width, :]) + mm(oh[rows, t_rows:], p_recv) + bias[...]
        )
    r_prev.wait()
    r_next.wait()
    r_w2.wait()
    p_send = mm(table[...], w1[width : 2 * width, :]).astype(BF16)
    for i in range(0, e_count, CHUNK):
        rows = pl.ds(i, CHUNK)
        value = pre[rows, :] + mm(oh[rows, :t_rows], p_send)
        pre[rows, :] = value
        active = (value * sigmoid(value)).astype(BF16)
        act[rows, :] = active
        norm, scale = normalize(mm(active, w2[...]))
        normed[rows, :] = norm
        scales[rows, :] = jnp.broadcast_to(scale, (CHUNK, 128))
        msg[rows, :] = (egain_v[...] * norm).astype(BF16)
    agg[0] = mm(oht[t_rows:, :], msg[...])
    r_agg = copies.remote(agg.at[0], agg.at[1], partner)
    c_n1.wait()
    c_n2.wait()
    c_ncot.wait()
    node_half = mm(nodes[...], n1[:width, :]) + nbias_v[...]
    nin[0] = nodes[...]
    r_agg.wait()
    gathered = (agg[0] + agg[1]).astype(BF16)
    nin[1] = gathered

    n_pre = node_half + mm(gathered, n1[width:, :])
    n_sig = sigmoid(n_pre)
    n_active = (n_pre * n_sig).astype(BF16)
    nact[...] = n_active
    n_norm, n_scale = normalize(mm(n_active, n2[...]))
    n_up = ncot[...].astype(F32)
    first_core = (1 - h).astype(F32)
    vec[...] = jnp.zeros_like(vec)
    vec[3:4, :] = jnp.sum(n_up * n_norm, axis=0, keepdims=True) * first_core
    n_dz = norm_back(n_up, ngain_v[...], n_norm, n_scale).astype(BF16)
    n_slope = n_sig * (1.0 + n_pre * (1.0 - n_sig))
    n_dh = (mm_nt(n_dz, n2[...]) * n_slope).astype(BF16)
    vec[2:3, :] = jnp.sum(n_dh.astype(F32), axis=0, keepdims=True) * first_core
    agg_grad = mm_nt(n_dh, n1[width:, :]).astype(BF16)
    my_feat = pl.ds(pl.multiple_of(h * half, 128), half)
    gnode[...] = ncot[:, my_feat].astype(F32) + mm_nt(n_dh, n1[my_feat, :])
    ngh = n_work
    grad = mm_tn(nin[h], n_dh).astype(BF16)
    for j in range(2):
        ngh[pl.ds(j * width, width), :] = grad[:, j * half : (j + 1) * half]
    grad = mm_tn(nact[:, my_hidden], n_dz).astype(BF16)
    for j in range(2):
        ngh[pl.ds(2 * width + j * hhalf, hhalf), :] = grad[:, j * half : (j + 1) * half]
    clear(ngh, 2 * width + 2 * hhalf)
    node_red = Reduction(copies, n_work, n_land, ng.at[h], node_rows_padded, steps)
    node_red.send_half(0)

    c_ecot.wait()
    gain_sum = jnp.zeros((1, width), F32)
    bias_sum = jnp.zeros((1, hid), F32)
    for i in range(0, e_count, CHUNK):
        rows = pl.ds(i, CHUNK)
        upstream = ecot[rows, :].astype(F32)
        norm = normed[rows, :]
        grad = upstream + mm(oh[rows, t_rows:], agg_grad)
        gain_sum = gain_sum + jnp.sum(grad * norm, axis=0, keepdims=True)
        d_z = norm_back(grad, egain_v[...], norm, scales[rows, 0:1]).astype(BF16)
        dz[rows, :] = d_z
        value = pre[rows, :]
        s = sigmoid(value)
        d_h = (mm_nt(d_z, w2[...]) * (s * (1.0 + value * (1.0 - s)))).astype(BF16)
        dh[rows, :] = d_h
        bias_sum = bias_sum + jnp.sum(d_h.astype(F32), axis=0, keepdims=True)
    vec[0:1, :] = bias_sum
    vec[1:2, :] = gain_sum
    r_vec = copies.remote(vec, vec_in.at[0], partner)
    grad = mm_tn(edges[...], dh[...])
    for j in range(2):
        gfirst[j] = grad[:, j * hhalf : (j + 1) * hhalf]
    gfirst_send[...] = gfirst[other].astype(BF16)
    r_first = copies.remote(gfirst_send, first_in, partner)
    gsecond[...] = mm_tn(act[...], dz[...])
    gsecond_send[...] = gsecond[pl.ds(pl.multiple_of(other * hhalf, 128), hhalf), :].astype(BF16)
    r_second = copies.remote(gsecond_send, second_in, partner)
    spart[...] = mm(oht[...], dh[...])
    s_send[...] = spart[...].astype(BF16)
    r_s = copies.remote(s_send, s_in, partner)
    node_red.advance()
    r_first.wait()
    top[pl.ds(0, width), :] = (gfirst[h] + first_in[...].astype(F32)).astype(BF16)
    r_second.wait()
    grad = (gsecond[my_hidden, :] + second_in[...].astype(F32)).astype(BF16)
    for j in range(2):
        top[pl.ds(width + j * hhalf, hhalf), :] = grad[:, j * half : (j + 1) * half]
    clear(top, width + 2 * hhalf)
    top_red = Reduction(copies, top, top_land, eg.at[0], edge_rows_padded, steps)
    top_red.send_half(0)
    node_red.advance()

    r_s.wait()
    spart[...] = spart[...] + s_in[...].astype(F32)
    s_all = spart[...].astype(BF16)
    t_grad = mm_nt(s_all[:t_rows], w1[pl.ds(pl.multiple_of(width + h * half, 128), half), :])
    back[...] = t_grad[n_count:].astype(BF16)
    r_back_prev = copies.remote(
        back.at[pl.ds(0, halo)], arriving.at[pl.ds(halo, halo)], prev
    )
    r_back_next = copies.remote(
        back.at[pl.ds(halo, halo)], arriving.at[pl.ds(0, halo)], after
    )
    gnode[...] = (
        gnode[...]
        + t_grad[:n_count]
        + mm_nt(s_all[t_rows:], w1[pl.ds(pl.multiple_of(2 * width + h * half, 128), half), :])
    )
    s_mine = spart[:, my_hidden].astype(BF16)
    low[pl.ds(0, width), :] = mm_tn(table[...], s_mine[:t_rows]).astype(BF16)
    low[pl.ds(width, width), :] = mm_tn(nodes[...], s_mine[t_rows:]).astype(BF16)
    clear(low, 2 * width)
    low_red = Reduction(copies, low, low_land, eg.at[1], edge_rows_padded, steps)
    low_red.send_half(0)
    node_red.advance()
    r_vec.wait()
    vec[...] = vec[...] + vec_in[0]
    count = len(steps)
    r_node = None
    c_top = []

    for i in range(0, e_count, CHUNK):
        rows = pl.ds(i, CHUNK)
        own = (ecot[rows, :].astype(F32) + mm_nt(dh[rows, :], w1[:width, :])).astype(BF16)
        for j in range(2):
            ge_half[j, rows, :] = own[:, j * half : (j + 1) * half]
    r_ge = copies.remote(ge_half.at[other], ge_full.at[my_rows], partner)
    c_ge = copies.local(ge_half.at[h], ge_full.at[my_rows])
    r_back_prev.wait()
    r_back_next.wait()
    gnode[...] = gnode[...] + (
        mm(pick_t[0], arriving[:halo]) + mm(pick_t[1], arriving[halo:])
    )
    back_out = gnode[...].astype(BF16)
    outgoing[:, :half] = back_out
    c_gn = copies.local(outgoing.at[:, pl.ds(0, half)], gn_out)
    r_ge.wait()
    c_ge.wait()
    c_geo = copies.local(ge_full, ge_out)

    r_vec = copies.remote(vec, vec_in.at[1], steps[0][0])
    top_red.advance()
    low_red.advance()
    for k in range(count):
        node_red.advance()
        top_red.advance()
        low_red.advance()
        r_vec.wait()
        vec[...] = vec[...] + vec_in[k + 1]
        if k + 1 < count:
            r_vec = copies.remote(vec, vec_in.at[k + 2], steps[k + 1][0])
    c_vec = copies.local(vec, vec_out)
    while not (node_red.done and top_red.done and low_red.done):
        node_red.advance()
        if node_red.done and r_node is None:
            r_node = copies.remote(ng.at[h], ng.at[h], partner)
        top_red.advance()
        if top_red.done and not c_top:
            c_top.append(copies.local(eg.at[0, pl.ds(0, width)], ef_out.at[pl.ds(0, width)]))
            for j in range(2):
                c_top.append(
                    copies.local(
                        eg.at[0, pl.ds(width + j * hhalf, hhalf)],
                        es_out.at[:, pl.ds(j * half, half)],
                    )
                )
        low_red.advance()
    c_low = copies.local(eg.at[1, pl.ds(0, 2 * width)], ef_out.at[pl.ds(width, 2 * width)])
    r_node.wait()
    for q in range(2):
        for j in range(2):
            c_top.append(
                copies.local(
                    ng.at[q, pl.ds(j * width, width)],
                    nf_out.at[pl.ds(q * width, width), pl.ds(j * half, half)],
                )
            )
            c_top.append(
                copies.local(
                    ng.at[q, pl.ds(2 * width + j * hhalf, hhalf)],
                    ns_out.at[pl.ds(q * hhalf, hhalf), pl.ds(j * half, half)],
                )
            )
    for copy in [c_gn, c_geo, c_vec, c_low] + c_top:
        copy.wait()


def on_device(
    mesh_sizes, nodes, edges, node_cotangent, edge_cotangent, senders, receivers, send_lists,
    edge_first, edge_bias, edge_second, edge_gain, node_first, node_bias, node_second, node_gain,
):
    batches, patches = mesh_sizes
    group = batches * patches
    n_count, width = nodes.shape[1:]
    e_all = edges.shape[1]
    e_count = e_all // 2
    hid = 2 * edge_second.shape[0]
    half, hhalf = width // 2, hid // 2
    halo = send_lists.shape[2]
    t_rows = n_count + 2 * halo
    unit = 16 * group
    n_rows = -(-(2 * width + 2 * hhalf) // unit) * unit
    e_rows = -(-max(2 * width, width + 2 * hhalf) // unit) * unit
    part = lax.axis_index("hidden")
    steps = group.bit_length() - 1
    row = lambda vector: vector[None, :]
    anywhere = pl.BlockSpec(memory_space=pl.ANY)
    inside = pl.BlockSpec(memory_space=pltpu.VMEM)
    V = pltpu.VMEM
    outs = pl.pallas_call(
        functools.partial(kernel, (batches, patches, n_rows, e_rows)),
        out_shape=(
            jax.ShapeDtypeStruct((n_count, half), BF16),
            jax.ShapeDtypeStruct((e_all, half), BF16),
            jax.ShapeDtypeStruct((3 * width, hhalf), BF16),
            jax.ShapeDtypeStruct((hhalf, width), BF16),
            jax.ShapeDtypeStruct((2 * width, hid), BF16),
            jax.ShapeDtypeStruct((hid, width), BF16),
            jax.ShapeDtypeStruct((8, width), F32),
        ),
        in_specs=[
            anywhere, anywhere, anywhere, anywhere, inside, inside, inside,
            anywhere, inside, anywhere, inside, anywhere, inside, anywhere, inside,
        ],
        out_specs=(anywhere,) * 7,
        scratch_shapes=[
            V((n_count, width), BF16),
            V((e_count, width), BF16),
            V((n_count, width), BF16),
            V((e_count, width), BF16),
            V((3 * width, hid), BF16),
            V((hid, width), BF16),
            V((2 * width, hid), BF16),
            V((hid, width), BF16),
            V((t_rows, width), BF16),
            V((2 * halo, width), BF16),
            V((t_rows + n_count, e_count), BF16),
            V((e_count, t_rows + n_count), BF16),
            V((e_count, hid), F32),
            V((e_count, hid), BF16),
            V((e_count, width), F32),
            V((e_count, 128), F32),
            V((e_count, width), BF16),
            V((2, n_count, width), F32),
            V((2, n_count, width), BF16),
            V((n_count, hid), BF16),
            V((e_count, width), BF16),
            V((e_count, hid), BF16),
            V((2, width, hhalf), F32),
            V((width, hhalf), BF16),
            V((hid, width), F32),
            V((hhalf, width), BF16),
            V((width, hhalf), BF16),
            V((hhalf, width), BF16),
            V((t_rows + n_count, hid), F32),
            V((t_rows + n_count, hid), BF16),
            V((t_rows + n_count, hid), BF16),
            V((2, e_count, half), BF16),
            V((e_all, half), BF16),
            V((2 * halo, half), BF16),
            V((2 * halo, half), BF16),
            V((n_count, half), F32),
            V((2, n_rows, half), BF16),
            V((n_rows, half), BF16),
            V((n_rows, half), BF16),
            V((2, e_rows, half), BF16),
            V((e_rows, half), BF16),
            V((e_rows, half), BF16),
            V((e_rows, half), BF16),
            V((e_rows, half), BF16),
            V((8, width), F32),
            V((steps + 1, 8, width), F32),
            V((1, hid), F32),
            pltpu.SemaphoreType.DMA((32,)),
            pltpu.SemaphoreType.DMA((16 + 7 * steps,)),
            pltpu.SemaphoreType.DMA((16 + 7 * steps,)),
        ],
        compiler_params=pltpu.CompilerParams(
            collective_id=0, has_side_effects=True, vmem_limit_bytes=60 * 1024 * 1024
        ),
    )(
        nodes[0], edges[0], node_cotangent[0], edge_cotangent[0],
        row(senders), row(receivers), send_lists[0],
        edge_first, row(edge_bias), edge_second, row(edge_gain),
        node_first, row(node_bias), node_second, row(node_gain),
    )
    g_nodes, g_edges, g_first, g_second, g_node_first, g_node_second, vec = outs
    return (
        g_nodes[None],
        g_edges[None],
        g_first.astype(F32),
        lax.dynamic_slice_in_dim(vec[0], part * hhalf, hhalf, 0),
        g_second.astype(F32),
        vec[1],
        g_node_first.astype(F32),
        vec[2],
        g_node_second.astype(F32),
        vec[3],
    )


def solution(mesh):
    placed = (
        P("batch", "space", None), P("batch", "space", None),
        P("batch", "space", None), P("batch", "space", None),
        P("space"), P("space"), P("space", None, None),
        P(None, "hidden"), P("hidden"), P("hidden", None),
        P(), P(), P(), P(), P(),
    )
    batches, patches = mesh.shape["batch"], mesh.shape["space"]
    assert mesh.shape["hidden"] == 2 and batches == 2
    assert patches & (patches - 1) == 0
    return jax.shard_map(
        functools.partial(on_device, (batches, patches)),
        mesh=mesh,
        in_specs=placed,
        out_specs=(
            P("batch", "space", "hidden"), P("batch", "space", "hidden"),
            P(None, "hidden"), P("hidden"), P("hidden", None),
            P(), P(), P(), P(), P(),
        ),
        check_vma=False,
    )
```
